256 devices in a mesh: dp: 128 (over y, x_hi, z, core), mp: 2 (over x_lo).
Axes of the slice: x: 4 (x_hi: 2, x_lo: 2; x = x_hi * 2 + x_lo), y: 4, z: 8, core: 2. Of those that a mesh axis runs over, the one named last changes fastest.
Arguments:
- dino_tokens: bfloat16 [65536, 1024], P('dp', 'mp'), may hold values from -6 to 6
- siglip_tokens: bfloat16 [65536, 1152], P('dp', 'mp'), may hold values from -6 to 6
- dino_norm_one: float32 [1024], replicated, may hold values from 0.25 to 1.75
- dino_qkv: bfloat16 [1024, 3, 1024], P('dp', None, 'mp'), may hold values from -6.05625 to 6.05625
- dino_out: bfloat16 [1024, 1024], P('mp', 'dp'), may hold values from -0.1875 to 0.1875
- dino_norm_two: float32 [1024], replicated, may hold values from 0.25 to 1.75
- dino_up: bfloat16 [1024, 4096], P('dp', 'mp'), may hold values from -0.1875 to 0.1875
- dino_down: bfloat16 [4096, 1024], P('mp', 'dp'), may hold values from -0.09375 to 0.09375
- siglip_norm_one: float32 [1152], replicated, may hold values from 0.25 to 1.75
- siglip_qkv: bfloat16 [1152, 3, 1152], P('dp', None, 'mp'), may hold values from -5.709887 to 5.709887
- siglip_out: bfloat16 [1152, 1152], P('mp', 'dp'), may hold values from -0.1875 to 0.1875
- siglip_norm_two: float32 [1152], replicated, may hold values from 0.25 to 1.75
- siglip_up: bfloat16 [1152, 4304], P('dp', 'mp'), may hold values from -0.1875 to 0.1875
- siglip_down: bfloat16 [4304, 1152], P('mp', 'dp'), may hold values from -0.09375 to 0.09375
Outputs:
- dino_result: bfloat16 [65536, 1024], P('dp', 'mp')
- siglip_result: bfloat16 [65536, 1152], P('dp', 'mp')
The draws below stay inside these ranges and needn't reach their ends.
All inputs are finite; a program needn't handle non-finite values.
Results may differ from the reference program's by a relative error of at most 0.012.
Values may be sent and summed in bfloat16 or wider, within the bound.
A program may use at most 128 MiB of HBM per device.

```python
import math
import jax
import jax.numpy as jnp
from jax import lax

D_DINO = 1024
FF_DINO = 4096
D_SIG = 1152
FF_SIG = 4304
HEADS = 16
PATCHES = 256
TOKENS = 65536


def qkv_law(key, width):
    first = jax.random.fold_in(key, 0)
    limit = 6.0 * width ** (-0.5)
    base = jnp.clip(jax.random.normal(first, (width, 3, width), jnp.float32) * width ** (-0.5), -limit, limit)
    return base


def draw_dino_qkv(key, part):
    return qkv_law(jax.random.fold_in(key, 11), D_DINO).astype(jnp.bfloat16)


def draw_siglip_qkv(key, part):
    return qkv_law(jax.random.fold_in(key, 23), D_SIG).astype(jnp.bfloat16)


def levels(rng, shape, cuts, low, high):
    factor_of, own = 1.0, jax.random.fold_in(rng, 6)
    for axis_at, shards_of in cuts:
        steps = jnp.exp(jax.random.uniform(jax.random.fold_in(own, axis_at), (shards_of,), jnp.float32, low / len(cuts), high / len(cuts)))
        factor_of = factor_of * jnp.repeat(steps, shape[axis_at] // shards_of).reshape([-1 if axis == axis_at else 1 for axis in range(len(shape))])
    return factor_of


def centred(own_key, extent, scale, reach, shards=(), held_as=jnp.bfloat16):
    drawn = scale * jax.random.normal(own_key, extent, jnp.float32)
    if shards:
        drawn = drawn * levels(own_key, extent, shards, -0.22, 0.18)
    return jnp.clip(drawn, -reach, reach).astype(held_as)


def setup_inputs(seed: int = 0) -> dict:
    arg_keys = jax.random.split(jax.random.key(seed), 15)
    return {
        "dino_tokens": centred(arg_keys[0], (TOKENS, D_DINO), 1.0, 6.0, ((0, 128), (1, 2))),
        "siglip_tokens": centred(arg_keys[1], (TOKENS, D_SIG), 1.0, 6.0, ((0, 128), (1, 2))),
        "dino_norm_one": jnp.clip(1.0 + 0.15 * jax.random.normal(arg_keys[2], (D_DINO,), jnp.float32), 0.25, 1.75),
        "dino_qkv": draw_dino_qkv(jax.random.fold_in(arg_keys[14], 71), 0),
        "dino_out": centred(arg_keys[4], (D_DINO, D_DINO), D_DINO ** -0.5, 0.1875, ((0, 2), (1, 128))),
        "dino_norm_two": jnp.clip(1.0 + 0.15 * jax.random.normal(arg_keys[5], (D_DINO,), jnp.float32), 0.25, 1.75),
        "dino_up": centred(arg_keys[6], (D_DINO, FF_DINO), D_DINO ** -0.5, 0.1875, ((0, 128), (1, 2))),
        "dino_down": centred(arg_keys[7], (FF_DINO, D_DINO), FF_DINO ** -0.5, 0.09375, ((0, 2), (1, 128))),
        "siglip_norm_one": jnp.clip(1.0 + 0.15 * jax.random.normal(arg_keys[8], (D_SIG,), jnp.float32), 0.25, 1.75),
        "siglip_qkv": draw_siglip_qkv(jax.random.fold_in(arg_keys[14], 71), 0),
        "siglip_out": centred(arg_keys[10], (D_SIG, D_SIG), D_SIG ** -0.5, 0.1875, ((0, 2), (1, 128))),
        "siglip_norm_two": jnp.clip(1.0 + 0.15 * jax.random.normal(arg_keys[11], (D_SIG,), jnp.float32), 0.25, 1.75),
        "siglip_up": centred(arg_keys[12], (D_SIG, FF_SIG), D_SIG ** -0.5, 0.1875, ((0, 128), (1, 2))),
        "siglip_down": centred(arg_keys[13], (FF_SIG, D_SIG), FF_SIG ** -0.5, 0.09375, ((0, 2), (1, 128))),
    }


EPS = 1e-06

def layer_norm(values, gain):
    values = values.astype(jnp.float32)
    center = values - lax.optimization_barrier(jnp.mean(values, axis=-1, keepdims=True))
    spread = lax.optimization_barrier(jnp.mean(center * center, axis=-1, keepdims=True))
    return (center * lax.rsqrt(spread + EPS) * gain.astype(jnp.float32)).astype(jnp.bfloat16)

def encode(block, norm_one, qkv_weight, out_weight, norm_two, up_weight, down_weight, approx):
    rows, width = block.shape
    head_size = width // HEADS
    scale = 1.0 / math.sqrt(head_size)
    normed = layer_norm(block, norm_one)
    qkv = jnp.dot(normed, qkv_weight.reshape(width, 3 * width), preferred_element_type=jnp.float32).astype(jnp.bfloat16)
    qkv = qkv.reshape(rows // PATCHES, PATCHES, 3, HEADS, head_size).astype(jnp.float32)
    query = qkv[:, :, 0]
    keys = qkv[:, :, 1]
    values = qkv[:, :, 2]
    scores = jnp.einsum('fqhd,fkhd->fhqk', query, keys) * scale
    top = lax.optimization_barrier(jnp.max(scores, axis=-1, keepdims=True))
    expo = jnp.exp(scores - top)
    probs = (expo / lax.optimization_barrier(jnp.sum(expo, axis=-1, keepdims=True))).astype(jnp.bfloat16)
    context = jnp.einsum('fhqk,fkhd->fqhd', probs.astype(jnp.float32), values)
    context = context.astype(jnp.bfloat16).reshape(rows, width)
    attended = jnp.dot(context, out_weight, preferred_element_type=jnp.float32)
    middle = (block.astype(jnp.float32) + attended).astype(jnp.bfloat16)
    second = layer_norm(middle, norm_two)
    hidden = jax.nn.gelu(jnp.dot(second, up_weight, preferred_element_type=jnp.float32), approximate=approx).astype(jnp.bfloat16)
    mixed = jnp.dot(hidden, down_weight, preferred_element_type=jnp.float32)
    return (middle.astype(jnp.float32) + mixed).astype(jnp.bfloat16)

def run_encoder(tokens, weights, approx):
    width = tokens.shape[1]
    blocks = tokens.reshape(-1, 8 * PATCHES, width)
    result = lax.map(lambda block: encode(block, *weights, approx), blocks)
    return result.reshape(tokens.shape)

def reference(dino_tokens, siglip_tokens, dino_norm_one, dino_qkv, dino_out, dino_norm_two, dino_up, dino_down, siglip_norm_one, siglip_qkv, siglip_out, siglip_norm_two, siglip_up, siglip_down):
    dino_result = run_encoder(dino_tokens, (dino_norm_one, dino_qkv, dino_out, dino_norm_two, dino_up, dino_down), False)
    siglip_result = run_encoder(siglip_tokens, (siglip_norm_one, siglip_qkv, siglip_out, siglip_norm_two, siglip_up, siglip_down), True)
    return (dino_result, siglip_result)
```

```python
import math

import jax
import jax.numpy as jnp
from jax import lax
from jax.sharding import PartitionSpec as P

HEADS = 16
PATCHES = 256
EPS = 1e-06


def from_everyone(shard, axis):
    size = lax.axis_size(axis)
    return lax.all_to_all(
        jnp.broadcast_to(shard[None], (size, *shard.shape)), axis, 0, 0, tiled=True
    )


def laid_out(pieces, dim):
    shape = list(pieces.shape[1:])
    shape[dim] *= pieces.shape[0]
    return jnp.moveaxis(pieces, 0, dim).reshape(shape)


def gathered_copies(shard, axis, dim):
    pieces = from_everyone(shard, axis)
    return laid_out(pieces, dim)


def split_up(shard, dim, size):
    shape = shard.shape
    pieces = shard.reshape(*shape[:dim], size, shape[dim] // size, *shape[dim + 1 :])
    return jnp.moveaxis(pieces, dim, 0)


def sum_at_owner(shard, axis, dim):
    pieces = split_up(shard, dim, lax.axis_size(axis))
    arrived = lax.all_to_all(pieces, axis, split_axis=0, concat_axis=0, tiled=True)
    return arrived.astype(jnp.float32).sum(axis=0)


def layer_norm(values, gain):
    values = values.astype(jnp.float32)
    center = values - jnp.mean(values, axis=-1, keepdims=True)
    spread = jnp.mean(center * center, axis=-1, keepdims=True)
    return (center * lax.rsqrt(spread + EPS) * gain).astype(jnp.bfloat16)


Y, XH, Z, C = 4, 2, 8, 2


def index(y, xh, z, c):
    return ((y * XH + xh) * Z + z) * C + c


PAIRS = [[index(y, xh, z, c) for xh in range(XH)] for y in range(Y) for z in range(Z) for c in range(C)]
PLANES = [[index(y, xh, z, c) for y in range(Y) for z in range(Z) for c in range(C)] for xh in range(XH)]


def gather_flat(parts):
    flat = jnp.concatenate([p.reshape(-1) for p in parts])
    count = flat.shape[0]
    rows = -(-count // 2048) * 16
    flat = jnp.pad(flat, (0, rows * 128 - count)).reshape(rows, 128)
    both = lax.all_gather(flat, "dp", axis=0, tiled=True, axis_index_groups=PAIRS)
    whole = lax.all_gather(both, "dp", axis=0, tiled=True, axis_index_groups=PLANES)
    whole = whole.reshape(Y, Z, C, XH, rows * 128).transpose(0, 3, 1, 2, 4).reshape(128, rows * 128)
    outs, at = [], 0
    for p in parts:
        outs.append(whole[:, at : at + p.size].reshape(128 * p.shape[0], p.size // p.shape[0]))
        at += p.size
    return outs


def attention_part(tokens, norm_one, qkv_weight, out_weight_t):
    rows, local_width = tokens.shape
    whole = gathered_copies(tokens, "mp", 1)
    width = whole.shape[1]
    head_size = width // HEADS
    local_heads = HEADS // 2
    scale = 1.0 / math.sqrt(head_size)
    normed = layer_norm(whole, norm_one)
    qkv = jnp.dot(normed, qkv_weight, preferred_element_type=jnp.float32)
    qkv = qkv.astype(jnp.bfloat16).reshape(rows // PATCHES, PATCHES, 3, local_heads, head_size)
    query = qkv[:, :, 0]
    keys = qkv[:, :, 1]
    values = qkv[:, :, 2]
    scores = jnp.einsum("fqhd,fkhd->fhqk", query, keys, preferred_element_type=jnp.float32) * scale
    top = jnp.max(scores, axis=-1, keepdims=True)
    expo = jnp.exp(scores - top)
    probs = (expo / jnp.sum(expo, axis=-1, keepdims=True)).astype(jnp.bfloat16)
    context = jnp.einsum("fhqk,fkhd->fqhd", probs, values, preferred_element_type=jnp.float32)
    context = context.astype(jnp.bfloat16).reshape(rows, local_heads * head_size)
    partial_attn = lax.dot_general(
        context, out_weight_t, (((1,), (1,)), ((), ())), preferred_element_type=jnp.float32
    )
    share = sum_at_owner(partial_attn.astype(jnp.bfloat16), "mp", 1)
    return (tokens.astype(jnp.float32) + share).astype(jnp.bfloat16)


def mlp_part(middle, norm_two, up_weight, down_weight_t, approx):
    middle_whole = gathered_copies(middle, "mp", 1)
    second = layer_norm(middle_whole, norm_two)
    raised = jnp.dot(second, up_weight, preferred_element_type=jnp.float32)
    hidden = jax.nn.gelu(raised, approximate=approx).astype(jnp.bfloat16)
    partial_mlp = lax.dot_general(
        hidden, down_weight_t, (((1,), (1,)), ((), ())), preferred_element_type=jnp.float32
    )
    mlp = sum_at_owner(partial_mlp.astype(jnp.bfloat16), "mp", 1)
    return (middle.astype(jnp.float32) + mlp).astype(jnp.bfloat16)


def local(
    dino_tokens,
    siglip_tokens,
    dino_norm_one,
    dino_qkv,
    dino_out,
    dino_norm_two,
    dino_up,
    dino_down,
    siglip_norm_one,
    siglip_qkv,
    siglip_out,
    siglip_norm_two,
    siglip_up,
    siglip_down,
):
    d_qkv, d_out, s_qkv, s_out = gather_flat(
        [dino_qkv.reshape(8, -1), dino_out.T, siglip_qkv.reshape(9, -1), siglip_out.T]
    )
    d_up, d_down, s_up, s_down = gather_flat([dino_up, dino_down.T, siglip_up, siglip_down.T])
    d_mid = attention_part(dino_tokens, dino_norm_one, d_qkv, d_out)
    s_mid = attention_part(siglip_tokens, siglip_norm_one, s_qkv, s_out)
    dino_result = mlp_part(d_mid, dino_norm_two, d_up, d_down, False)
    siglip_result = mlp_part(s_mid, siglip_norm_two, s_up, s_down, True)
    return (dino_result, siglip_result)


def solution(mesh):
    in_specs = (
        P("dp", "mp"),
        P("dp", "mp"),
        P(),
        P("dp", None, "mp"),
        P("mp", "dp"),
        P(),
        P("dp", "mp"),
        P("mp", "dp"),
        P(),
        P("dp", None, "mp"),
        P("mp", "dp"),
        P(),
        P("dp", "mp"),
        P("mp", "dp"),
    )
    out_specs = (P("dp", "mp"), P("dp", "mp"))
    return jax.shard_map(local, mesh=mesh, in_specs=in_specs, out_specs=out_specs, check_vma=False)
```

```python
import functools
import heapq
import math

import jax
import jax.numpy as jnp
from jax import lax
from jax.experimental import pallas as pl
from jax.experimental.pallas import tpu as pltpu
from jax.sharding import PartitionSpec as P

HEADS = 16
LOCAL = HEADS // 2
PATCHES = 256
EPS = 1e-06
BF = jnp.bfloat16
F32 = jnp.float32

Y, XH, Z, C = 4, 2, 8, 2


RING = {"y": Y, "z": Z}


def onward(order, piece):
    dy, dz, dx, half = piece
    place = {"y": dy, "z": dz}

    def ring(axis):
        d, n = place[axis], RING[axis]

        def at(to, h):
            spot = dict(place, **{axis: to})
            return (spot["y"], spot["z"], dx, h)

        if d == 0:
            return [(axis + "+", at(-1, half)), (axis + "-", at(1, half))]
        if d < 0 and -d < n // 2 - 1:
            return [(axis + "+", at(d - 1, half))]
        if d > 0 and d < n // 2 - 1:
            return [(axis + "-", at(d + 1, half))]
        if d == 1 - n // 2 and half != 1:
            return [(axis + "+", at(-n // 2, 0))]
        if d == n // 2 - 1 and half != 0:
            return [(axis + "-", at(-n // 2, 1))]
        return []

    first, second = order
    sends = ring(first) if place[second] == 0 else []
    return sends + ring(second)


def arrivals(streams, rate=0.044, hop=2.0, across=9.0):
    free = dict.fromkeys(("y+", "y-", "z+", "z-"), 0.0)
    events, order = [], []
    for s in range(len(streams)):
        events += [(0.0, len(events), s, (0, 0, 0, None)), (across, len(events) + 1, s, (0, 0, 1, None))]
    heapq.heapify(events)
    count = len(events)
    while events:
        t, _, s, piece = heapq.heappop(events)
        order.append((s, piece))
        for link, child in onward(streams[s][0], piece):
            size = streams[s][2] * (1.0 if child[3] is None else 0.5)
            free[link] = max(free[link], t) + size * rate
            count += 1
            heapq.heappush(events, (free[link] + hop, count, s, child))
    return order


def gather_kernel(streams, order, block, dino, siglip, w, dino_got, siglip_got, send, recv, pass_send, pass_recv, more_send, more_recv, near):
    me, mp = lax.axis_index("dp"), lax.axis_index("mp")
    c, z, xh, y = lax.rem(me, 2), lax.rem(me // 2, 8), lax.rem(me // 16, 2), me // 32

    def at(y, xh, z, c):
        return ((y * XH + xh) * Z + z) * C + c

    up_y, down_y = lax.rem(y + 1, Y), lax.rem(y + Y - 1, Y)
    up_z, down_z = lax.rem(z + 1, Z), lax.rem(z + Z - 1, Z)
    to = {
        "y+": (at(up_y, xh, z, c), mp),
        "y-": (at(down_y, xh, z, c), mp),
        "z+": (at(y, xh, up_z, c), mp),
        "z-": (at(y, xh, down_z, c), mp),
        "x": (at(y, 1 - xh, z, c), mp),
        "core": (at(y, xh, z, 1 - c), mp),
        "mp": (me, 1 - mp),
    }
    number = {event: i for i, event in enumerate(order)}

    def columns(s, half):
        _, start, tiles = streams[s]
        low, high = {None: (0, tiles), 0: (0, tiles // 2), 1: (tiles // 2, tiles)}[half]
        return slice((start + low) * 128, (start + high) * 128)

    def spot(s, piece, half=None):
        dy, dz, dx, mine = piece
        half = mine if half is None else half
        source = (lax.rem(y + dy + Y, Y), lax.rem(z + dz + Z, Z), c, lax.rem(xh + dx, 2))
        return w.at[(*source, slice(None), columns(s, half))]

    def remote(src, dst, sends, receives, k, link):
        return pltpu.make_async_remote_copy(
            src_ref=src,
            dst_ref=dst,
            send_sem=sends.at[k],
            recv_sem=receives.at[k],
            device_id=to[link],
            device_id_type=pl.DeviceIdType.MESH,
        )

    def source_of(s, piece, half):
        if piece[:3] == (0, 0, 0):
            return block.at[:, columns(s, half)]
        return spot(s, piece, half)

    def hop(s, piece, link, child):
        return remote(source_of(s, piece, child[3]), spot(s, piece, child[3]), send, recv, number[(s, child)], link)

    def share(s, piece):
        k = number[(s, piece)]
        return remote(source_of(s, piece, piece[3]), spot(s, piece), pass_send, pass_recv, k, "core")

    def arrived(s, piece):
        k = number[(s, piece)]
        return remote(spot(s, piece), spot(s, piece), send, recv, k, "y+")

    barrier = pltpu.get_barrier_semaphore()
    for device in to.values():
        pl.semaphore_signal(barrier, inc=1, device_id=device, device_id_type=pl.DeviceIdType.MESH)
    pl.semaphore_wait(barrier, len(to))

    own = [s for s in range(len(streams))]
    across = [hop(s, (0, 0, 0, None), "x", (0, 0, 1, None)) for s in own]
    tokens = [
        remote(dino, dino_got, more_send, more_recv, 0, "mp"),
        remote(siglip, siglip_got, more_send, more_recv, 1, "mp"),
    ]
    for copy in across:
        copy.start()
    started = []
    for i, (s, piece) in enumerate(order):
        if piece != (0, 0, 0, None):
            arrived(s, piece).wait_recv()
        for link, child in onward(streams[s][0], piece):
            copy = hop(s, piece, link, child)
            copy.start()
            started.append(copy)
        copy = share(s, piece)
        copy.start()
        if i == len(streams) - 1:
            for copy in tokens:
                copy.start()
            mine = pltpu.make_async_copy(block, w.at[y, z, c, xh], near)
            mine.start()
    for copy in started + across:
        copy.wait_send()
    for s, piece in order:
        copy = share(s, piece)
        copy.wait_send()
        dy, dz, dx, half = piece
        source = (lax.rem(y + dy + Y, Y), lax.rem(z + dz + Z, Z), 1 - c, lax.rem(xh + dx, 2))
        there = w.at[(*source, slice(None), columns(s, half))]
        remote(there, there, pass_send, pass_recv, number[(s, piece)], "core").wait_recv()
    for copy in tokens:
        copy.wait()
    mine.wait()


def gather(block, dino, siglip, split):
    tiles = block.shape[1] // 128
    streams = (("yz", 0, split), ("zy", split, tiles - split))
    order = arrivals(streams)
    hbm = pl.BlockSpec(memory_space=pl.ANY)
    dma = pltpu.SemaphoreType.DMA
    n = len(order)
    w, dino_got, siglip_got = pl.pallas_call(
        functools.partial(gather_kernel, streams, order),
        out_shape=(
            jax.ShapeDtypeStruct((Y, Z, C, XH, *block.shape), BF),
            jax.ShapeDtypeStruct(dino.shape, BF),
            jax.ShapeDtypeStruct(siglip.shape, BF),
        ),
        in_specs=[pl.BlockSpec(memory_space=pltpu.VMEM), hbm, hbm],
        out_specs=(hbm, hbm, hbm),
        scratch_shapes=[dma((n,)), dma((n,)), dma((n,)), dma((n,)), dma((2,)), dma((2,)), dma],
        compiler_params=pltpu.CompilerParams(
            collective_id=0, has_side_effects=True, vmem_limit_bytes=16 << 20
        ),
        cost_estimate=pl.CostEstimate(flops=1 << 30, bytes_accessed=32 << 20, transcendentals=0),
        name="gather",
    )(block, dino, siglip)
    return w.reshape(1024, block.shape[1]), dino_got, siglip_got


def widen(x, to):
    return jnp.pad(x, ((0, 0), (0, to - x.shape[1])))


def extra_block(rows, widths, columns):
    flat = jnp.concatenate([widen(r, w).reshape(-1) for r, w in zip(rows, widths)])
    return jnp.pad(flat, (0, 8 * columns - flat.shape[0])).reshape(8, columns)


def one_hot(per_device):
    width = 64 * per_device
    held = lax.broadcasted_iota(jnp.int32, (width, width), 1)
    slot = jnp.where(held < 512, held // 8, held - 512)
    row = jnp.where(held < 512, held % 8, 8)
    xh, c, z, y = slot % 2, (slot // 2) % 2, (slot // 4) % 8, slot // 32
    natural = (((y * XH + xh) * Z + z) * C + c) * per_device + row
    return (lax.broadcasted_iota(jnp.int32, (width, width), 0) == natural).astype(BF)


def held_gain(gain, per_device):
    parts = gain.reshape(Y, XH, Z, C, per_device).transpose(0, 2, 3, 1, 4).reshape(128, per_device)
    held = parts[:, :8].reshape(-1)
    if per_device == 9:
        held = jnp.concatenate([held, parts[:, 8]])
    return held.reshape(1, -1)


def both_halves(mine, other, low):
    a = jnp.where(low, mine, other)
    b = jnp.where(low, other, mine)
    return jnp.concatenate([a[:, :512], b[:, :512], a[:, 512:], b[:, 512:]], axis=1)


def half_of(whole, first):
    low = jnp.concatenate([whole[:, :512], whole[:, 1024 : 1024 + (whole.shape[1] - 1024) // 2]], axis=1)
    high = jnp.concatenate([whole[:, 512:1024], whole[:, 1024 + (whole.shape[1] - 1024) // 2 :]], axis=1)
    return jnp.where(first, low, high)


def swap(x):
    return lax.ppermute(x, "mp", [(0, 1), (1, 0)])


def normed(x, gain):
    center = x - jnp.mean(x, axis=-1, keepdims=True)
    spread = jnp.mean(center * center, axis=-1, keepdims=True)
    return (center * lax.rsqrt(spread + EPS) * gain).astype(BF)


def dot(a, b):
    return jnp.dot(a, b, preferred_element_type=F32)


def dot_t(a, b):
    return lax.dot_general(a, b, (((1,), (1,)), ((), ())), preferred_element_type=F32)


def gelu(x, approx):
    if approx:
        return jax.nn.gelu(x, approximate=True)
    half = 0.5 * x
    return half + half * lax.erf(x * math.sqrt(0.5))


def attention_kernel(size, at_qkv, n_qkv, at_out, n_out, extra, *refs):
    if extra:
        x_ref, g_ref, w_ref, eq_ref, eo_ref, o_ref, wq, wo, sems = refs
    else:
        x_ref, g_ref, w_ref, o_ref, wq, wo, sems = refs
    first = pltpu.make_async_copy(w_ref.at[:, at_qkv : at_qkv + n_qkv], wq, sems.at[0])
    second = pltpu.make_async_copy(w_ref.at[:, at_out : at_out + n_out], wo, sems.at[1])
    first.start()
    second.start()
    first.wait()
    second.wait()
    scale = 1.0 / math.sqrt(size)
    mine = LOCAL * size

    def frame(f, carry):
        rows = pl.ds(pl.multiple_of(f * PATCHES, PATCHES), PATCHES)
        x = normed(x_ref[rows, :].astype(F32), g_ref[...])
        qkv = dot(x[:, :1024], wq[...])
        if extra:
            qkv = qkv + dot(x[:, 1024:], eq_ref[...])
        qkv = qkv.astype(BF)
        heads = []
        for h in range(LOCAL):
            q, k, v = (qkv[:, j * mine + h * size : j * mine + (h + 1) * size] for j in range(3))
            s = dot_t(q, k)
            e = jnp.exp((s - jnp.max(s, axis=-1, keepdims=True)) * scale)
            total = jnp.sum(e, axis=-1, keepdims=True)
            heads.append((dot(e.astype(BF), v) / total).astype(BF))
        if n_out > mine:
            heads.append(jnp.zeros((PATCHES, n_out - mine), BF))
        ctx = jnp.concatenate(heads, axis=1)
        o_ref[rows, :1024] = dot_t(ctx, wo[...]).astype(BF)
        if extra:
            o_ref[rows, 1024:] = dot_t(ctx, eo_ref[...]).astype(BF)
        return carry

    lax.fori_loop(0, 2, frame, 0)


def attention(x, gain, w, extras, size, at_qkv, n_qkv, at_out, n_out):
    vmem = pl.BlockSpec(memory_space=pltpu.VMEM)
    flops = 2 * x.shape[0] * x.shape[1] * (n_qkv + n_out) + 4 * 2 * LOCAL * PATCHES * PATCHES * size
    return pl.pallas_call(
        functools.partial(attention_kernel, size, at_qkv, n_qkv, at_out, n_out, bool(extras)),
        out_shape=jax.ShapeDtypeStruct(x.shape, BF),
        in_specs=[vmem, vmem, pl.BlockSpec(memory_space=pl.ANY)] + [vmem] * len(extras),
        out_specs=vmem,
        scratch_shapes=[
            pltpu.VMEM((1024, n_qkv), BF),
            pltpu.VMEM((1024, n_out), BF),
            pltpu.SemaphoreType.DMA((2,)),
        ],
        compiler_params=pltpu.CompilerParams(vmem_limit_bytes=48 << 20),
        cost_estimate=pl.CostEstimate(flops=flops, bytes_accessed=8 << 20, transcendentals=1 << 20),
        name="attention",
    )(x, gain, w, *extras)


def mlp_kernel(steps, approx, extra, *refs):
    if extra:
        low_ref, x_ref, p_ref, r_ref, g_ref, u_ref, d_ref, ue_ref, de_ref, keep_ref, send_ref, mid, second, acc = refs
    else:
        low_ref, x_ref, p_ref, r_ref, g_ref, u_ref, d_ref, keep_ref, send_ref, mid, second, acc = refs
    j = pl.program_id(0)

    @pl.when(j == 0)
    def _():
        def rows_of(i, carry):
            rows = pl.ds(pl.multiple_of(i * 128, 128), 128)
            m = x_ref[rows, :].astype(F32) + (p_ref[rows, :].astype(F32) + r_ref[rows, :].astype(F32))
            m = m.astype(BF)
            mid[rows, :] = m
            second[rows, :] = normed(m.astype(F32), g_ref[...])
            return carry

        lax.fori_loop(0, 4, rows_of, 0)

    def rows_of(i, carry):
        rows = pl.ds(pl.multiple_of(i * 256, 256), 256)
        raised = dot(second[rows, :1024], u_ref[...])
        if extra:
            raised = raised + dot(second[rows, 1024:], ue_ref[...])
        hidden = gelu(raised, approx).astype(BF)
        main = dot_t(hidden, d_ref[...])
        rest = dot_t(hidden, de_ref[...]) if extra else None

        @pl.when(j == 0)
        def _():
            acc[rows, :1024] = main
            if extra:
                acc[rows, 1024:] = rest

        @pl.when(j > 0)
        def _():
            acc[rows, :1024] += main
            if extra:
                acc[rows, 1024:] += rest

        return carry

    lax.fori_loop(0, 2, rows_of, 0)

    @pl.when(j == steps - 1)
    def _():
        low = low_ref[0] == 0

        def rows_of(i, carry):
            rows = pl.ds(pl.multiple_of(i * 128, 128), 128)
            part = acc[rows, :]
            m = mid[rows, :].astype(F32)

            def put(keep_at, send_at):
                keep_ref[rows, :512] = m[:, keep_at : keep_at + 512] + part[:, keep_at : keep_at + 512]
                send_ref[rows, :512] = part[:, send_at : send_at + 512].astype(BF)
                if extra:
                    ka, sa = 1024 + keep_at // 8, 1024 + send_at // 8
                    keep_ref[rows, 512:] = m[:, ka : ka + 64] + part[:, ka : ka + 64]
                    send_ref[rows, 512:] = part[:, sa : sa + 64].astype(BF)

            @pl.when(low)
            def _():
                put(0, 512)

            @pl.when(jnp.logical_not(low))
            def _():
                put(512, 0)

            return carry

        lax.fori_loop(0, 4, rows_of, 0)


def mlp(mp, x, part, arrived, gain, w, extras, approx, chunk, steps, at):
    rows, width = x.shape
    half = width // 2
    whole = lambda shape: pl.BlockSpec(shape, lambda j, s: (0, 0))
    in_specs = [whole((rows, width))] * 3 + [whole((1, width))]
    in_specs += [
        pl.BlockSpec((1024, chunk), lambda j, s: (0, at // chunk + j)),
        pl.BlockSpec((1024, chunk), lambda j, s: (0, at // chunk + steps + j)),
    ]
    in_specs += [pl.BlockSpec((128, chunk), lambda j, s: (0, j))] * len(extras)
    flops = 4 * rows * width * chunk * steps
    return pl.pallas_call(
        functools.partial(mlp_kernel, steps, approx, bool(extras)),
        out_shape=(jax.ShapeDtypeStruct((rows, half), F32), jax.ShapeDtypeStruct((rows, half), BF)),
        grid_spec=pltpu.PrefetchScalarGridSpec(
            num_scalar_prefetch=1,
            grid=(steps,),
            in_specs=in_specs,
            out_specs=(whole((rows, half)), whole((rows, half))),
            scratch_shapes=[
                pltpu.VMEM((rows, width), BF),
                pltpu.VMEM((rows, width), BF),
                pltpu.VMEM((rows, width), F32),
            ],
        ),
        compiler_params=pltpu.CompilerParams(
            dimension_semantics=("arbitrary",), vmem_limit_bytes=56 << 20
        ),
        cost_estimate=pl.CostEstimate(flops=flops, bytes_accessed=12 << 20, transcendentals=1 << 20),
        name="mlp",
    )(mp, x, part, arrived, gain, w, w, *extras)


def local(
    dino_tokens,
    siglip_tokens,
    dino_norm_one,
    dino_qkv,
    dino_out,
    dino_norm_two,
    dino_up,
    dino_down,
    siglip_norm_one,
    siglip_qkv,
    siglip_out,
    siglip_norm_two,
    siglip_up,
    siglip_down,
):
    mp = lax.axis_index("mp")
    low = mp == 0
    mp_word = mp.reshape(1).astype(jnp.int32)

    d_out_t, d_down_t = dino_out.T, dino_down.T
    s_qkv = siglip_qkv.reshape(9, -1)
    s_out_t, s_down_t = siglip_out.T, siglip_down.T
    block_one = jnp.concatenate(
        [
            dino_qkv.reshape(8, -1),
            d_out_t,
            widen(s_qkv[:8], 1792),
            widen(s_out_t[:8], 640),
            extra_block([s_qkv[8:], s_out_t[8:]], [1792, 640], 384),
        ],
        axis=1,
    )
    block_two = jnp.concatenate(
        [
            widen(siglip_up[:8], 2304),
            widen(s_down_t[:8], 2304),
            dino_up,
            d_down_t,
            extra_block([siglip_up[8:], s_down_t[8:]], [2304, 2304], 640),
        ],
        axis=1,
    )
    d_hot, s_hot = one_hot(8), one_hot(9)
    d_mine = dot(dino_tokens, d_hot).astype(BF)
    s_mine = dot(siglip_tokens, s_hot).astype(BF)
    w, d_other, s_other = gather(jnp.concatenate([block_two, block_one], axis=1), d_mine, s_mine, 44)
    d_whole = both_halves(d_mine, d_other, low)
    s_whole = both_halves(s_mine, s_other, low)

    s_extra = w[:, 13824:14208].reshape(128, 3072)
    d_part = attention(d_whole, held_gain(dino_norm_one, 8), w, (), 64, 9344, 1536, 10880, 512)
    d_arrived = swap(d_part)
    s_part = attention(
        s_whole, held_gain(siglip_norm_one, 9), w, (s_extra[:, :1792], s_extra[:, 1792:2432]), 72, 11392, 1792, 13184, 640
    )
    s_arrived = swap(s_part)

    s_extra_two = w[:, 8704:9344].reshape(128, 5120)
    d_keep, d_send = mlp(mp_word, d_whole, d_part, d_arrived, held_gain(dino_norm_two, 8), w, (), False, 512, 4, 4608)
    d_got = swap(d_send)
    s_keep, s_send = mlp(
        mp_word,
        s_whole,
        s_part,
        s_arrived,
        held_gain(siglip_norm_two, 9),
        w,
        (s_extra_two[:, :2304], s_extra_two[:, 2304:4608]),
        True,
        768,
        3,
        0,
    )
    s_got = swap(s_send)
    dino_result = dot_t((d_keep + d_got.astype(F32)).astype(BF), d_hot).astype(BF)
    siglip_result = dot_t((s_keep + s_got.astype(F32)).astype(BF), s_hot).astype(BF)
    return (dino_result, siglip_result)


def solution(mesh):
    in_specs = (
        P("dp", "mp"),
        P("dp", "mp"),
        P(),
        P("dp", None, "mp"),
        P("mp", "dp"),
        P(),
        P("dp", "mp"),
        P("mp", "dp"),
        P(),
        P("dp", None, "mp"),
        P("mp", "dp"),
        P(),
        P("dp", "mp"),
        P("mp", "dp"),
    )
    out_specs = (P("dp", "mp"), P("dp", "mp"))
    return jax.shard_map(local, mesh=mesh, in_specs=in_specs, out_specs=out_specs, check_vma=False)
```

```python
import functools
import heapq
import math

import jax
import jax.numpy as jnp
from jax import lax
from jax.experimental import pallas as pl
from jax.experimental.pallas import tpu as pltpu
from jax.sharding import PartitionSpec as P

HEADS = 16
LOCAL = HEADS // 2
PATCHES = 256
EPS = 1e-06
BF = jnp.bfloat16
F32 = jnp.float32

Y, XH, Z, C = 4, 2, 8, 2


RING = {"y": Y, "z": Z}


def onward(order, piece):
    dy, dz, dx, half = piece
    place = {"y": dy, "z": dz}

    def ring(axis):
        d, n = place[axis], RING[axis]

        def at(to, h):
            spot = dict(place, **{axis: to})
            return (spot["y"], spot["z"], dx, h)

        if d == 0:
            return [(axis + "+", at(-1, half)), (axis + "-", at(1, half))]
        if d < 0 and -d < n // 2 - 1:
            return [(axis + "+", at(d - 1, half))]
        if d > 0 and d < n // 2 - 1:
            return [(axis + "-", at(d + 1, half))]
        if d == 1 - n // 2 and half != 1:
            return [(axis + "+", at(-n // 2, 0))]
        if d == n // 2 - 1 and half != 0:
            return [(axis + "-", at(-n // 2, 1))]
        return []

    first, second = order
    sends = ring(first) if place[second] == 0 else []
    return sends + ring(second)


def schedule(streams, tasks, rate=0.05, hop=2.5, across=10.0, issue=0.08, shallow=1.5, deep=10.0):
    free = dict.fromkeys(("y+", "y-", "z+", "z-"), 0.0)
    pending = {link: [] for link in free}
    coming, program, count, now, done = [], [], 0, 0.0, 0
    for s in range(len(streams)):
        heapq.heappush(coming, (0.0, count, s, (0, 0, 0, None)))
        heapq.heappush(coming, (across, count + 1, s, (0, 0, 1, None)))
        count += 2
    first = [s for s, stream in enumerate(streams) if stream[3] == 0]
    left = sum(1 for s in first for _ in range(2 * 43))
    complete = None
    while coming or any(pending.values()):
        task = tasks[done] if done < len(tasks) else None
        ready = task is not None and now >= task[0] and (not task[1] or (complete is not None and now >= complete + 3.0))
        depth = deep if complete is not None and task is not None else shallow
        for link, queue in pending.items():
            while queue and free[link] - now < depth:
                _, _, s, piece, child = heapq.heappop(queue)
                program.append(("send", s, piece, link, child))
                now += issue
                size = streams[s][2] * (1.0 if child[3] is None else 0.5)
                free[link] = max(free[link], now) + size * rate
                count += 1
                heapq.heappush(coming, (free[link] + hop, count, s, child))
        if ready:
            slack = [free[link] - now for link in free]
            if sum(min(x, task[2]) for x in slack) >= 0.55 * 4 * task[2] or not coming or coming[0][0] > now + 1.0:
                program.append(("task", done))
                now += task[2]
                done += 1
                continue
        if not coming:
            now += 0.2
            continue
        t, _, s, piece = heapq.heappop(coming)
        now = max(now, t) + issue
        program.append(("wait", s, piece))
        if s in first:
            left -= 1
            if left == 0:
                complete = now
        for link, child in onward(streams[s][0], piece):
            count += 1
            heapq.heappush(pending[link], (streams[s][3], count, s, piece, child))
    comm = now
    for k in range(done, len(tasks)):
        program.append(("task", k))
        now += tasks[k][2]
    return program, complete, comm, now


TASKS = [(0.0, False, 2.0), (30.0, False, 1.5), (0.0, True, 0.5), (0.0, True, 1.0)]
TASKS += [(0.0, True, d) for d in (2.5, 2.6, 1.6) * 2] + [(40.0, True, 1.2)] + [(0.0, True, d) for d in (2.2, 2.0, 1.2) * 2]
UP_S, UP_D, REST_TWO, QKV_D, OUT_D, QKV_S, OUT_S, REST_ONE, END = 0, 4608, 8704, 9344, 10880, 11392, 13184, 13824, 14208


def layer_kernel(
    streams, program, d_qkv, d_out, d_up, d_down, s_qkv, s_out, s_up, s_down, dino, siglip, dino_one, dino_two, siglip_one, siglip_two, dino_out, siglip_out,
    send, recv, pass_send, pass_recv, more_send, more_recv,
    w, dino_x, siglip_x, dino_part, siglip_part, dino_got, siglip_got, dino_gain, siglip_gain,
    block, dino_in, siglip_in, hot_d, hot_s, rest_q, rest_o, qkv_buf, ctx_buf,
    rest_two, second, acc, keep_d, keep_s, sent_d, sent_s, back_d, back_s,
):
    me, mp = lax.axis_index("dp"), lax.axis_index("mp")
    c, z, xh, y = lax.rem(me, 2), lax.rem(me // 2, 8), lax.rem(me // 16, 2), me // 32
    low = mp == 0

    def at(y, xh, z, c):
        return ((y * XH + xh) * Z + z) * C + c

    up_y, down_y = lax.rem(y + 1, Y), lax.rem(y + Y - 1, Y)
    up_z, down_z = lax.rem(z + 1, Z), lax.rem(z + Z - 1, Z)
    to = {
        "y+": (at(up_y, xh, z, c), mp),
        "y-": (at(down_y, xh, z, c), mp),
        "z+": (at(y, xh, up_z, c), mp),
        "z-": (at(y, xh, down_z, c), mp),
        "x": (at(y, 1 - xh, z, c), mp),
        "core": (at(y, xh, z, 1 - c), mp),
        "mp": (me, 1 - mp),
    }
    timeline = [step[1:] for step in program if step[0] == "wait"]
    number = {event: i for i, event in enumerate(timeline)}

    def columns(s, half):
        _, start, tiles, _ = streams[s]
        first, last = {None: (0, tiles), 0: (0, tiles // 2), 1: (tiles // 2, tiles)}[half]
        return slice((start + first) * 128, (start + last) * 128)

    def spot(s, piece, half=None, core=None):
        dy, dz, dx, mine = piece
        half = mine if half is None else half
        source = (lax.rem(y + dy + Y, Y), lax.rem(z + dz + Z, Z), c if core is None else core, lax.rem(xh + dx, 2))
        return w.at[(*source, slice(None), columns(s, half))]

    def remote(src, dst, sends, receives, k, link):
        return pltpu.make_async_remote_copy(
            src_ref=src,
            dst_ref=dst,
            send_sem=sends.at[k],
            recv_sem=receives.at[k],
            device_id=to[link],
            device_id_type=pl.DeviceIdType.MESH,
        )

    def source_of(s, piece, half):
        if piece[:3] == (0, 0, 0):
            return block.at[:, columns(s, half)]
        return spot(s, piece, half)

    def hop(s, piece, link, child):
        return remote(source_of(s, piece, child[3]), spot(s, piece, child[3]), send, recv, number[(s, child)], link)

    def share(s, piece):
        return remote(source_of(s, piece, piece[3]), spot(s, piece), pass_send, pass_recv, number[(s, piece)], "core")

    def arrived(s, piece):
        return remote(spot(s, piece), spot(s, piece), send, recv, number[(s, piece)], "y+")

    def shared(s, piece):
        there = spot(s, piece, core=1 - c)
        return remote(there, there, pass_send, pass_recv, number[(s, piece)], "core")

    barrier = pltpu.get_barrier_semaphore()
    for device in to.values():
        pl.semaphore_signal(barrier, inc=1, device_id=device, device_id_type=pl.DeviceIdType.MESH)
    for start, width, mine in ((UP_S, 2304, s_up), (UP_S + 2304, 2304, s_down), (QKV_S, 1792, s_qkv), (OUT_S, 640, s_out)):
        got = mine.shape[1]
        block[:, start : start + got] = mine[:8, :]
        block[:, start + got : start + width] = jnp.zeros((8, width - got), BF)
    for i in range(3):
        block[:, QKV_D + i * 512 : QKV_D + (i + 1) * 512] = d_qkv[i]
    block[:, OUT_D:QKV_S] = d_out[...]
    block[:, UP_D : UP_D + 2048] = d_up[...]
    block[:, UP_D + 2048 : REST_TWO] = d_down[...]
    for start, width, mine in ((REST_ONE, 384, ((s_qkv, 1792), (s_out, 640))), (REST_TWO, 640, ((s_up, 2304), (s_down, 2304)))):
        ninth, long = [], 8 * width
        for ref, to_width in mine:
            ninth += [ref[8:9, :], jnp.zeros((1, to_width - ref.shape[1]), BF)]
            long -= to_width
        ninth = jnp.concatenate([*ninth, jnp.zeros((1, long), BF)], axis=1)
        for r in range(8):
            block[r : r + 1, start : start + width] = ninth[:, r * width : (r + 1) * width]
    pl.semaphore_wait(barrier, len(to))

    across = [hop(s, (0, 0, 0, None), "x", (0, 0, 1, None)) for s in range(len(streams))]
    tokens_s = remote(siglip, siglip_in, more_send, more_recv, 0, "mp")
    tokens_d = remote(dino, dino_in, more_send, more_recv, 1, "mp")
    for copy in across:
        copy.start()
    tokens_s.start()
    tokens_d.start()
    started, parts = list(across), []

    def matrix(start, stop):
        return w[:, :, :, :, :, start:stop].reshape(1024, stop - start)

    def chosen(r):
        rows, columns = (lax.broadcasted_iota(jnp.int32, (128, 1024), axis) for axis in range(2))
        return (columns == rows * 8 + r).astype(BF)

    def begin():
        w[y, z, c, xh] = block[...]
        hot_d[...] = one_hot(8)
        hot_s[...] = one_hot(9)
        for one, two, hot, out in ((dino_one, dino_two, hot_d, dino_gain), (siglip_one, siglip_two, hot_s, siglip_gain)):
            half = hot.shape[0]
            gains = jnp.concatenate([one[:, :half], two[:, :half], one[:, half:], two[:, half:]], axis=0)
            held = jnp.dot(gains, hot[...].astype(F32), preferred_element_type=F32, precision=lax.Precision.HIGHEST)
            out[:, :512], out[:, 512:1024] = held[0:2, :512], held[2:4, :512]
            if out.shape[1] > 1024:
                out[:, 1024:1088], out[:, 1088:] = held[0:2, 512:], held[2:4, 512:]

    def pick(ref, rows, hot):
        if ref.shape[0] == hot.shape[0] and ref.shape[1] != hot.shape[0]:
            return lax.dot_general(ref[:, rows], hot[...], (((0,), (0,)), ((), ())), preferred_element_type=F32).astype(BF)
        return dot(ref[rows, :], hot[...]).astype(BF)

    def place(ref, other, hot, out, copy):
        def go():
            copy.wait_recv()
            for i in range(2):
                rows = slice(i * 256, (i + 1) * 256)
                held, far = pick(ref, rows, hot), pick(other, rows, hot)
                first, second = jnp.where(low, held, far), jnp.where(low, far, held)
                out[rows, :512], out[rows, 512:1024] = first[:, :512], second[:, :512]
                if out.shape[1] > 1024:
                    out[rows, 1024:] = jnp.concatenate([first[:, 512:], second[:, 512:]], axis=1)

        return go

    early = [s for s, stream in enumerate(streams) if stream[3] == 0]

    def load():
        for s, piece in timeline:
            if s in early:
                shared(s, piece).wait_recv()

    def ready_s():
        block_rest = matrix(REST_ONE, END)
        for r in range(8):
            got = dot(chosen(r), block_rest).astype(BF)
            start = r * 384
            if start + 384 <= 1792:
                rest_q[:, start : start + 384] = got
            elif start < 1792:
                rest_q[:, start:] = got[:, : 1792 - start]
                rest_o[:, : start + 384 - 1792] = got[:, 1792 - start :]
            elif start < 2432:
                stop = min(start + 384, 2432)
                rest_o[:, start - 1792 : stop - 1792] = got[:, : stop - start]

    def project(x, gain, wq, more, n):
        def go(f):
            rows = slice(f * PATCHES, (f + 1) * PATCHES)
            v = normed(x[rows, :].astype(F32), gain[0:1, :])
            qkv = dot(v[:, :1024], matrix(*wq))
            if more is not None:
                qkv = qkv + dot(v[:, 1024:], more[...])
            qkv_buf[:, :n] = qkv.astype(BF)

        return go

    def attend(size, n):
        def go(f):
            scale, held = 1.0 / math.sqrt(size), LOCAL * size
            qkv = qkv_buf[:, : 3 * held]
            heads = []
            for h in range(LOCAL):
                q, k, v = (qkv[:, j * held + h * size : j * held + (h + 1) * size] for j in range(3))
                s = dot_t(q, k)
                e = jnp.exp((s - jnp.max(s, axis=-1, keepdims=True)) * scale)
                total = jnp.sum(e, axis=-1, keepdims=True)
                heads.append((dot(e.astype(BF), v) / total).astype(BF))
            if n > held:
                heads.append(jnp.zeros((PATCHES, n - held), BF))
            ctx_buf[:, :n] = jnp.concatenate(heads, axis=1)

        return go

    def leave(wo, more, n, part, got, k):
        def go(f):
            rows = slice(f * PATCHES, (f + 1) * PATCHES)
            ctx = ctx_buf[:, :n]
            part[rows, :1024] = dot_t(ctx, matrix(*wo)).astype(BF)
            if more is not None:
                part[rows, 1024:] = dot_t(ctx, more[...]).astype(BF)
            parts.append(remote(part.at[rows], got.at[rows], more_send, more_recv, k + f, "mp"))

        return go

    steps_s = [project(siglip_x, siglip_gain, (QKV_S, OUT_S), rest_q, 1792), attend(72, 640), leave((OUT_S, REST_ONE), rest_o, 640, siglip_part, siglip_got, 2)]
    steps_d = [project(dino_x, dino_gain, (QKV_D, OUT_D), None, 1536), attend(64, 512), leave((OUT_D, QKV_S), None, 512, dino_part, dino_got, 4)]
    work = [begin, place(siglip, siglip_in, hot_s, siglip_x, tokens_s), load, ready_s]
    work += [functools.partial(go, f) for f in range(2) for go in steps_s]
    work += [place(dino, dino_in, hot_d, dino_x, tokens_d)]
    work += [functools.partial(go, f) for f in range(2) for go in steps_d]

    sent = 0
    for kind, *step in program:
        while sent < len(parts):
            parts[sent].start()
            sent += 1
        if kind == "task":
            work[step[0]]()
        elif kind == "send":
            s, piece, link, child = step
            started.append(hop(s, piece, link, child))
            started[-1].start()
        else:
            s, piece = step
            if piece[:3] != (0, 0, 0):
                arrived(s, piece).wait_recv()
            share(s, piece).start()
    while sent < len(parts):
        parts[sent].start()
        sent += 1
    for copy in started:
        copy.wait_send()
    for s, piece in timeline:
        share(s, piece).wait_send()
        if s not in early:
            shared(s, piece).wait_recv()
    tokens_s.wait_send()
    tokens_d.wait_send()
    for copy in parts:
        copy.wait()

    for r in range(8):
        rest_two[:, r * 640 : (r + 1) * 640] = dot(chosen(r), matrix(REST_TWO, QKV_D)).astype(BF)

    def columns(start, j, chunk):
        return pl.ds(pl.multiple_of(start + j * chunk, 128), chunk)

    def mlp(x, part, got, gain, at, chunk, steps, approx, keep, out, back, k):
        extra = x.shape[1] > 1024

        def rows_of(i, carry):
            rows = pl.ds(pl.multiple_of(i * 256, 256), 256)
            m = x[rows, :].astype(F32) + (part[rows, :].astype(F32) + got[rows, :].astype(F32))
            m = m.astype(BF)
            x[rows, :] = m
            second[:, : x.shape[1]] = normed(m.astype(F32), gain[1:2, :])
            acc[...] = jnp.zeros_like(acc)

            def chunk_of(j, carry):
                up = w[:, :, :, :, :, columns(at, j, chunk)].reshape(1024, chunk)
                down = w[:, :, :, :, :, columns(at + steps * chunk, j, chunk)].reshape(1024, chunk)
                raised = dot(second[:, :1024], up)
                if extra:
                    raised = raised + dot(second[:, 1024:], rest_two[:, columns(0, j, chunk)])
                hidden = gelu(raised, approx).astype(BF)
                acc[:, :1024] += dot_t(hidden, down)
                if extra:
                    acc[:, 1024:] += dot_t(hidden, rest_two[:, columns(steps * chunk, j, chunk)])
                return carry

            lax.fori_loop(0, steps, chunk_of, 0)

            def put(keep_at, send_at):
                keep[rows, :512] = x[rows, keep_at : keep_at + 512].astype(F32) + acc[:, keep_at : keep_at + 512]
                out[rows, :512] = acc[:, send_at : send_at + 512].astype(BF)
                if extra:
                    ka, sa = 1024 + keep_at // 8, 1024 + send_at // 8
                    keep[rows, 512:] = x[rows, ka : ka + 64].astype(F32) + acc[:, ka : ka + 64]
                    out[rows, 512:] = acc[:, sa : sa + 64].astype(BF)

            @pl.when(low)
            def _():
                put(0, 512)

            @pl.when(jnp.logical_not(low))
            def _():
                put(512, 0)

            remote(out.at[rows], back.at[rows], more_send, more_recv, k + i, "mp").start()
            return carry

        lax.fori_loop(0, 2, rows_of, 0)

    mlp(siglip_x, siglip_part, siglip_got, siglip_gain, UP_S, 768, 3, True, keep_s, sent_s, back_s, 6)
    mlp(dino_x, dino_part, dino_got, dino_gain, UP_D, 512, 4, False, keep_d, sent_d, back_d, 8)
    for keep, out, back, k in ((keep_s, sent_s, back_s, 6), (keep_d, sent_d, back_d, 8)):
        for i in range(2):
            rows = slice(i * 256, (i + 1) * 256)
            remote(out.at[rows], back.at[rows], more_send, more_recv, k + i, "mp").wait()
            result = (keep[rows, :] + back[rows, :].astype(F32)).astype(BF)
            if k == 6:
                siglip_out[:, rows] = dot_t(hot_s[...], result).astype(BF)
            else:
                dino_out[rows, :] = dot_t(result, hot_d[...]).astype(BF)


def layer(shards, dino, siglip, *gains):
    streams = (
        ("yz", QKV_D // 128, 13, 0),
        ("zy", QKV_D // 128 + 13, 25, 0),
        ("yz", 0, 28, 1),
        ("zy", 28, 45, 1),
    )
    program = schedule(streams, TASKS)[0]
    vmem = pl.BlockSpec(memory_space=pltpu.VMEM)
    dma = pltpu.SemaphoreType.DMA
    n = sum(step[0] == "wait" for step in program)
    rows = dino.shape[0]
    wide = lambda width, height=rows, dtype=BF: pltpu.VMEM((height, width), dtype)
    return pl.pallas_call(
        functools.partial(layer_kernel, streams, program),
        out_shape=(jax.ShapeDtypeStruct(dino.shape, BF), jax.ShapeDtypeStruct(siglip.shape, BF)),
        in_specs=[vmem] * 14,
        out_specs=(vmem, vmem),
        scratch_shapes=[
            dma((n,)), dma((n,)), dma((n,)), dma((n,)), dma((10,)), dma((10,)),
            pltpu.VMEM((Y, Z, C, XH, 8, END), BF),
            wide(1024), wide(1152), wide(1024), wide(1152), wide(1024), wide(1152), wide(1024, 2, F32), wide(1152, 2, F32),
            wide(END, 8), wide(512), pltpu.VMEM(siglip.shape, BF), wide(512, 512), wide(576, 576),
            wide(1792, 128), wide(640, 128), wide(1792, PATCHES), wide(640, PATCHES),
            wide(5120, 128), wide(1152, 256), wide(1152, 256, F32),
            wide(512, rows, F32), wide(576, rows, F32), wide(512), wide(576), wide(512), wide(576),
        ],
        compiler_params=pltpu.CompilerParams(
            collective_id=0, has_side_effects=True, vmem_limit_bytes=67043328
        ),
        cost_estimate=pl.CostEstimate(flops=1 << 34, bytes_accessed=32 << 20, transcendentals=1 << 22),
        name="layer",
    )(*shards, dino, siglip, *gains)


def one_hot(per_device):
    width = 64 * per_device
    held = lax.broadcasted_iota(jnp.int32, (width, width), 1)
    slot = jnp.where(held < 512, held // 8, held - 512)
    row = jnp.where(held < 512, held % 8, 8)
    xh, c, z, y = slot % 2, (slot // 2) % 2, (slot // 4) % 8, slot // 32
    natural = (((y * XH + xh) * Z + z) * C + c) * per_device + row
    return (lax.broadcasted_iota(jnp.int32, (width, width), 0) == natural).astype(BF)


def normed(x, gain):
    center = x - jnp.mean(x, axis=-1, keepdims=True)
    spread = jnp.mean(center * center, axis=-1, keepdims=True)
    return (center * lax.rsqrt(spread + EPS) * gain).astype(BF)


def dot(a, b):
    return jnp.dot(a, b, preferred_element_type=F32)


def dot_t(a, b):
    return lax.dot_general(a, b, (((1,), (1,)), ((), ())), preferred_element_type=F32)


def gelu(x, approx):
    if approx:
        return jax.nn.gelu(x, approximate=True)
    half = 0.5 * x
    return half + half * lax.erf(x * math.sqrt(0.5))


def local(
    dino_tokens,
    siglip_tokens,
    dino_norm_one,
    dino_qkv,
    dino_out,
    dino_norm_two,
    dino_up,
    dino_down,
    siglip_norm_one,
    siglip_qkv,
    siglip_out,
    siglip_norm_two,
    siglip_up,
    siglip_down,
):
    shards = [
        dino_qkv.transpose(1, 0, 2), dino_out.T, dino_up, dino_down.T,
        siglip_qkv.reshape(9, -1), siglip_out.T, siglip_up, siglip_down.T,
    ]
    gains = [g.reshape(1, -1) for g in (dino_norm_one, dino_norm_two, siglip_norm_one, siglip_norm_two)]
    dino_result, siglip_result = layer(shards, dino_tokens, siglip_tokens.T, *gains)
    return (dino_result, siglip_result.T)


def solution(mesh):
    in_specs = (
        P("dp", "mp"),
        P("dp", "mp"),
        P(),
        P("dp", None, "mp"),
        P("mp", "dp"),
        P(),
        P("dp", "mp"),
        P("mp", "dp"),
        P(),
        P("dp", None, "mp"),
        P("mp", "dp"),
        P(),
        P("dp", "mp"),
        P("mp", "dp"),
    )
    out_specs = (P("dp", "mp"), P("dp", "mp"))
    return jax.shard_map(local, mesh=mesh, in_specs=in_specs, out_specs=out_specs, check_vma=False)
```

```python
import functools
import heapq
import math

import jax
import jax.numpy as jnp
from jax import lax
from jax.experimental import pallas as pl
from jax.experimental.pallas import tpu as pltpu
from jax.sharding import PartitionSpec as P

HEADS = 16
LOCAL = HEADS // 2
PATCHES = 256
EPS = 1e-06
BF = jnp.bfloat16
F32 = jnp.float32

Y, XH, Z, C = 4, 2, 8, 2


RING = {"y": Y, "z": Z}


def onward(order, piece):
    dy, dz, dx, half = piece
    place = {"y": dy, "z": dz}

    def ring(axis):
        d, n = place[axis], RING[axis]

        def at(to, h):
            spot = dict(place, **{axis: to})
            return (spot["y"], spot["z"], dx, h)

        if d == 0:
            return [(axis + "+", at(-1, half)), (axis + "-", at(1, half))]
        if d < 0 and -d < n // 2 - 1:
            return [(axis + "+", at(d - 1, half))]
        if d > 0 and d < n // 2 - 1:
            return [(axis + "-", at(d + 1, half))]
        if d == 1 - n // 2 and half != 1:
            return [(axis + "+", at(-n // 2, 0))]
        if d == n // 2 - 1 and half != 0:
            return [(axis + "-", at(-n // 2, 1))]
        return []

    first, second = order
    sends = ring(first) if place[second] == 0 else []
    return sends + ring(second)


def schedule(streams, tasks, rate=0.05, hop=2.5, across=10.0, issue=0.08, shallow=1.5, deep=10.0):
    free = dict.fromkeys(("y+", "y-", "z+", "z-"), 0.0)
    pending = {link: [] for link in free}
    coming, program, count, now, done = [], [], 0, 0.0, 0
    for s in range(len(streams)):
        heapq.heappush(coming, (0.0, count, s, (0, 0, 0, None)))
        heapq.heappush(coming, (across, count + 1, s, (0, 0, 1, None)))
        count += 2
    first = [s for s, stream in enumerate(streams) if stream[3] == 0]
    left = sum(1 for s in first for _ in range(2 * 43))
    complete = None
    while coming or any(pending.values()):
        task = tasks[done] if done < len(tasks) else None
        ready = task is not None and now >= task[0] and (not task[1] or (complete is not None and now >= complete + 3.0))
        depth = deep if complete is not None and task is not None else shallow
        for link, queue in pending.items():
            while queue and free[link] - now < depth:
                _, _, s, piece, child = heapq.heappop(queue)
                program.append(("send", s, piece, link, child))
                now += issue
                size = streams[s][2] * (1.0 if child[3] is None else 0.5)
                free[link] = max(free[link], now) + size * rate
                count += 1
                heapq.heappush(coming, (free[link] + hop, count, s, child))
        if ready:
            slack = [free[link] - now for link in free]
            if sum(min(x, task[2]) for x in slack) >= 0.55 * 4 * task[2] or not coming or coming[0][0] > now + 1.0:
                program.append(("task", done))
                now += task[2]
                done += 1
                continue
        if not coming:
            now += 0.2
            continue
        t, _, s, piece = heapq.heappop(coming)
        now = max(now, t) + issue
        program.append(("wait", s, piece))
        if s in first:
            left -= 1
            if left == 0:
                complete = now
        for link, child in onward(streams[s][0], piece):
            count += 1
            heapq.heappush(pending[link], (streams[s][3], count, s, piece, child))
    comm = now
    for k in range(done, len(tasks)):
        program.append(("task", k))
        now += tasks[k][2]
    return program, complete, comm, now


TASKS = [(0.0, False, 2.0), (30.0, False, 1.5), (0.0, True, 0.5), (0.0, True, 1.0)]
TASKS += [(0.0, True, d) for d in (2.5, 2.6, 1.6) * 2] + [(40.0, True, 1.2)] + [(0.0, True, d) for d in (2.2, 2.0, 1.2) * 2]
UP_S, UP_D, REST_TWO, QKV_D, OUT_D, QKV_S, OUT_S, REST_ONE, END = 0, 4608, 8704, 9344, 10880, 11392, 13184, 13824, 14208


def layer_kernel(
    streams, program, d_qkv, d_out, d_up, d_down, s_qkv, s_out, s_up, s_down, dino, siglip, dino_one, dino_two, siglip_one, siglip_two, dino_out, siglip_out,
    send, recv, pass_send, pass_recv, more_send, more_recv,
    w, dino_x, siglip_x, dino_part, siglip_part, dino_got, siglip_got, dino_gain, siglip_gain,
    block, dino_in, siglip_in, hot_d, hot_s, rest_q, rest_o, qkv_buf, ctx_buf,
    rest_two, second, hidden, acc, keep_d, keep_s, sent_d, sent_s, back_d, back_s,
):
    me, mp = lax.axis_index("dp"), lax.axis_index("mp")
    c, z, xh, y = lax.rem(me, 2), lax.rem(me // 2, 8), lax.rem(me // 16, 2), me // 32
    low = mp == 0

    def at(y, xh, z, c):
        return ((y * XH + xh) * Z + z) * C + c

    up_y, down_y = lax.rem(y + 1, Y), lax.rem(y + Y - 1, Y)
    up_z, down_z = lax.rem(z + 1, Z), lax.rem(z + Z - 1, Z)
    to = {
        "y+": (at(up_y, xh, z, c), mp),
        "y-": (at(down_y, xh, z, c), mp),
        "z+": (at(y, xh, up_z, c), mp),
        "z-": (at(y, xh, down_z, c), mp),
        "x": (at(y, 1 - xh, z, c), mp),
        "core": (at(y, xh, z, 1 - c), mp),
        "mp": (me, 1 - mp),
    }
    timeline = [step[1:] for step in program if step[0] == "wait"]
    number = {event: i for i, event in enumerate(timeline)}

    def columns(s, half):
        _, start, tiles, _ = streams[s]
        first, last = {None: (0, tiles), 0: (0, tiles // 2), 1: (tiles // 2, tiles)}[half]
        return slice((start + first) * 128, (start + last) * 128)

    def spot(s, piece, half=None, core=None):
        dy, dz, dx, mine = piece
        half = mine if half is None else half
        source = (lax.rem(y + dy + Y, Y), lax.rem(z + dz + Z, Z), c if core is None else core, lax.rem(xh + dx, 2))
        return w.at[(*source, slice(None), columns(s, half))]

    def remote(src, dst, sends, receives, k, link):
        return pltpu.make_async_remote_copy(
            src_ref=src,
            dst_ref=dst,
            send_sem=sends.at[k],
            recv_sem=receives.at[k],
            device_id=to[link],
            device_id_type=pl.DeviceIdType.MESH,
        )

    def source_of(s, piece, half):
        if piece[:3] == (0, 0, 0):
            return block.at[:, columns(s, half)]
        return spot(s, piece, half)

    def hop(s, piece, link, child):
        return remote(source_of(s, piece, child[3]), spot(s, piece, child[3]), send, recv, number[(s, child)], link)

    def share(s, piece):
        return remote(source_of(s, piece, piece[3]), spot(s, piece), pass_send, pass_recv, number[(s, piece)], "core")

    def arrived(s, piece):
        return remote(spot(s, piece), spot(s, piece), send, recv, number[(s, piece)], "y+")

    def shared(s, piece):
        there = spot(s, piece, core=1 - c)
        return remote(there, there, pass_send, pass_recv, number[(s, piece)], "core")

    barrier = pltpu.get_barrier_semaphore()
    for device in to.values():
        pl.semaphore_signal(barrier, inc=1, device_id=device, device_id_type=pl.DeviceIdType.MESH)
    for start, width, mine in ((UP_S, 2304, s_up), (UP_S + 2304, 2304, s_down), (QKV_S, 1792, s_qkv), (OUT_S, 640, s_out)):
        got = mine.shape[1]
        block[:, start : start + got] = mine[:8, :]
        block[:, start + got : start + width] = jnp.zeros((8, width - got), BF)
    for i in range(3):
        block[:, QKV_D + i * 512 : QKV_D + (i + 1) * 512] = d_qkv[i]
    block[:, OUT_D:QKV_S] = d_out[...]
    block[:, UP_D : UP_D + 2048] = d_up[...]
    block[:, UP_D + 2048 : REST_TWO] = d_down[...]
    for start, width, mine in ((REST_ONE, 384, ((s_qkv, 1792), (s_out, 640))), (REST_TWO, 640, ((s_up, 2304), (s_down, 2304)))):
        ninth, long = [], 8 * width
        for ref, to_width in mine:
            ninth += [ref[8:9, :], jnp.zeros((1, to_width - ref.shape[1]), BF)]
            long -= to_width
        ninth = jnp.concatenate([*ninth, jnp.zeros((1, long), BF)], axis=1)
        for r in range(8):
            block[r : r + 1, start : start + width] = ninth[:, r * width : (r + 1) * width]
    pl.semaphore_wait(barrier, len(to))

    across = [hop(s, (0, 0, 0, None), "x", (0, 0, 1, None)) for s in range(len(streams))]
    tokens_s = remote(siglip, siglip_in, more_send, more_recv, 0, "mp")
    tokens_d = remote(dino, dino_in, more_send, more_recv, 1, "mp")
    for copy in across:
        copy.start()
    tokens_s.start()
    tokens_d.start()
    started, parts = list(across), []

    def matrix(start, stop):
        return w[:, :, :, :, :, start:stop].reshape(1024, stop - start)

    def chosen(r):
        rows, columns = (lax.broadcasted_iota(jnp.int32, (128, 1024), axis) for axis in range(2))
        return (columns == rows * 8 + r).astype(BF)

    def begin():
        w[y, z, c, xh] = block[...]
        hot_d[...] = one_hot(8)
        hot_s[...] = one_hot(9)
        for one, two, hot, out in ((dino_one, dino_two, hot_d, dino_gain), (siglip_one, siglip_two, hot_s, siglip_gain)):
            half = hot.shape[0]
            gains = jnp.concatenate([one[:, :half], two[:, :half], one[:, half:], two[:, half:]], axis=0)
            held = jnp.dot(gains, hot[...].astype(F32), preferred_element_type=F32, precision=lax.Precision.HIGHEST)
            out[:, :512], out[:, 512:1024] = held[0:2, :512], held[2:4, :512]
            if out.shape[1] > 1024:
                out[:, 1024:1088], out[:, 1088:] = held[0:2, 512:], held[2:4, 512:]

    def pick(ref, rows, hot):
        if ref.shape[0] == hot.shape[0] and ref.shape[1] != hot.shape[0]:
            return lax.dot_general(ref[:, rows], hot[...], (((0,), (0,)), ((), ())), preferred_element_type=F32).astype(BF)
        return dot(ref[rows, :], hot[...]).astype(BF)

    def place(ref, other, hot, out, copy):
        def go():
            copy.wait_recv()
            for i in range(2):
                rows = slice(i * 256, (i + 1) * 256)
                held, far = pick(ref, rows, hot), pick(other, rows, hot)
                first, second = jnp.where(low, held, far), jnp.where(low, far, held)
                out[rows, :512], out[rows, 512:1024] = first[:, :512], second[:, :512]
                if out.shape[1] > 1024:
                    out[rows, 1024:] = jnp.concatenate([first[:, 512:], second[:, 512:]], axis=1)

        return go

    early = [s for s, stream in enumerate(streams) if stream[3] == 0]

    def load():
        for s, piece in timeline:
            if s in early:
                shared(s, piece).wait_recv()

    def ready_s():
        block_rest = matrix(REST_ONE, END)
        for r in range(8):
            got = dot(chosen(r), block_rest).astype(BF)
            start = r * 384
            if start + 384 <= 1792:
                rest_q[:, start : start + 384] = got
            elif start < 1792:
                rest_q[:, start:] = got[:, : 1792 - start]
                rest_o[:, : start + 384 - 1792] = got[:, 1792 - start :]
            elif start < 2432:
                stop = min(start + 384, 2432)
                rest_o[:, start - 1792 : stop - 1792] = got[:, : stop - start]

    def project(x, gain, wq, more, n):
        def go(f):
            rows = slice(f * PATCHES, (f + 1) * PATCHES)
            v = normed(x[rows, :].astype(F32), gain[0:1, :])
            qkv = dot(v[:, :1024], matrix(*wq))
            if more is not None:
                qkv = qkv + dot(v[:, 1024:], more[...])
            qkv_buf[:, :n] = qkv.astype(BF)

        return go

    def attend(size, n):
        def go(f):
            scale, held = 1.0 / math.sqrt(size), LOCAL * size
            qkv = qkv_buf[:, : 3 * held]
            heads = []
            for h in range(LOCAL):
                q, k, v = (qkv[:, j * held + h * size : j * held + (h + 1) * size] for j in range(3))
                s = dot_t(q, k)
                e = jnp.exp((s - jnp.max(s, axis=-1, keepdims=True)) * scale)
                total = jnp.sum(e, axis=-1, keepdims=True)
                heads.append((dot(e.astype(BF), v) / total).astype(BF))
            if n > held:
                heads.append(jnp.zeros((PATCHES, n - held), BF))
            ctx_buf[:, :n] = jnp.concatenate(heads, axis=1)

        return go

    def leave(wo, more, n, part, got, k):
        def go(f):
            rows = slice(f * PATCHES, (f + 1) * PATCHES)
            ctx = ctx_buf[:, :n]
            part[rows, :1024] = dot_t(ctx, matrix(*wo)).astype(BF)
            if more is not None:
                part[rows, 1024:] = dot_t(ctx, more[...]).astype(BF)
            parts.append(remote(part.at[rows], got.at[rows], more_send, more_recv, k + f, "mp"))

        return go

    steps_s = [project(siglip_x, siglip_gain, (QKV_S, OUT_S), rest_q, 1792), attend(72, 640), leave((OUT_S, REST_ONE), rest_o, 640, siglip_part, siglip_got, 2)]
    steps_d = [project(dino_x, dino_gain, (QKV_D, OUT_D), None, 1536), attend(64, 512), leave((OUT_D, QKV_S), None, 512, dino_part, dino_got, 4)]
    work = [begin, place(siglip, siglip_in, hot_s, siglip_x, tokens_s), load, ready_s]
    work += [functools.partial(go, f) for f in range(2) for go in steps_s]
    work += [place(dino, dino_in, hot_d, dino_x, tokens_d)]
    work += [functools.partial(go, f) for f in range(2) for go in steps_d]

    sent = 0
    for kind, *step in program:
        while sent < len(parts):
            parts[sent].start()
            sent += 1
        if kind == "task":
            work[step[0]]()
        elif kind == "send":
            s, piece, link, child = step
            started.append(hop(s, piece, link, child))
            started[-1].start()
        else:
            s, piece = step
            if piece[:3] != (0, 0, 0):
                arrived(s, piece).wait_recv()
            share(s, piece).start()
    while sent < len(parts):
        parts[sent].start()
        sent += 1
    for copy in started:
        copy.wait_send()
    for s, piece in timeline:
        share(s, piece).wait_send()
        if s not in early:
            shared(s, piece).wait_recv()
    tokens_s.wait_send()
    tokens_d.wait_send()
    for copy in parts:
        copy.wait()

    for r in range(8):
        rest_two[:, r * 640 : (r + 1) * 640] = dot(chosen(r), matrix(REST_TWO, QKV_D)).astype(BF)

    def span(start, j, chunk):
        return pl.ds(pl.multiple_of(start + j * chunk, 128), chunk)

    def mlp(x, part, got, gain, at, inner, chunk, approx, keep, out, back, k):
        extra, width = x.shape[1] > 1024, x.shape[1]

        def begin(i, carry):
            rows = pl.ds(pl.multiple_of(i * 128, 128), 128)
            m = x[rows, :].astype(F32) + (part[rows, :].astype(F32) + got[rows, :].astype(F32))
            m = m.astype(BF)
            x[rows, :] = m
            second[rows, :width] = normed(m.astype(F32), gain[1:2, :])
            return carry

        lax.fori_loop(0, 4, begin, 0)

        def lift(j, carry):
            up = w[:, :, :, :, :, span(at, j, 256)].reshape(1024, 256)
            raised = dot(second[:, :1024], up)
            if extra:
                raised = raised + dot(second[:, 1024:], rest_two[:, span(0, j, 256)])
            hidden[:, span(0, j, 256)] = gelu(raised, approx).astype(BF)
            return carry

        lax.fori_loop(0, inner // 256, lift, 0)

        def lower(which, before):
            acc[...] = jnp.zeros_like(acc)
            before()

            def add(j, carry):
                h = hidden[:, span(0, j, chunk)]
                down = w[pl.ds(2 * which, 2), :, :, :, :, span(at + inner, j, chunk)].reshape(512, chunk)
                acc[:, :512] += dot_t(h, down)
                if extra:
                    more = rest_two[pl.ds(pl.multiple_of(which * 64, 64), 64), span(inner, j, chunk)]
                    acc[:, 512:] += dot_t(h, more)
                return carry

            lax.fori_loop(0, inner // chunk, add, 0)

        lower(1 - mp, lambda: None)
        out[...] = acc[:, : out.shape[1]].astype(BF)
        lower(mp, lambda: remote(out, back, more_send, more_recv, k, "mp").start())
        keep[:, :512] = x[:, span(0, mp, 512)].astype(F32) + acc[:, :512]
        if extra:
            keep[:, 512:] = jnp.where(low, x[:, 1024:1088], x[:, 1088:]).astype(F32) + acc[:, 512:]

    mlp(siglip_x, siglip_part, siglip_got, siglip_gain, UP_S, 2304, 768, True, keep_s, sent_s, back_s, 6)
    mlp(dino_x, dino_part, dino_got, dino_gain, UP_D, 2048, 1024, False, keep_d, sent_d, back_d, 7)
    for keep, out, back, k in ((keep_s, sent_s, back_s, 6), (keep_d, sent_d, back_d, 7)):
        remote(out, back, more_send, more_recv, k, "mp").wait()
        for i in range(2):
            rows = slice(i * 256, (i + 1) * 256)
            result = (keep[rows, :] + back[rows, :].astype(F32)).astype(BF)
            if k == 6:
                siglip_out[:, rows] = dot_t(hot_s[...], result).astype(BF)
            else:
                dino_out[rows, :] = dot_t(result, hot_d[...]).astype(BF)


def layer(shards, dino, siglip, *gains):
    streams = (
        ("yz", QKV_D // 128, 13, 0),
        ("zy", QKV_D // 128 + 13, 25, 0),
        ("yz", 0, 28, 1),
        ("zy", 28, 45, 1),
    )
    program = schedule(streams, TASKS)[0]
    vmem = pl.BlockSpec(memory_space=pltpu.VMEM)
    dma = pltpu.SemaphoreType.DMA
    n = sum(step[0] == "wait" for step in program)
    rows = dino.shape[0]
    wide = lambda width, height=rows, dtype=BF: pltpu.VMEM((height, width), dtype)
    return pl.pallas_call(
        functools.partial(layer_kernel, streams, program),
        out_shape=(jax.ShapeDtypeStruct(dino.shape, BF), jax.ShapeDtypeStruct(siglip.shape, BF)),
        in_specs=[vmem] * 14,
        out_specs=(vmem, vmem),
        scratch_shapes=[
            dma((n,)), dma((n,)), dma((n,)), dma((n,)), dma((8,)), dma((8,)),
            pltpu.VMEM((Y, Z, C, XH, 8, END), BF),
            wide(1024), wide(1152), wide(1024), wide(1152), wide(1024), wide(1152), wide(1024, 2, F32), wide(1152, 2, F32),
            wide(END, 8), wide(512), pltpu.VMEM(siglip.shape, BF), wide(512, 512), wide(576, 576),
            wide(1792, 128), wide(640, 128), wide(1792, PATCHES), wide(640, PATCHES),
            wide(5120, 128), wide(1152), wide(2304), wide(576, rows, F32),
            wide(512, rows, F32), wide(576, rows, F32), wide(512), wide(576), wide(512), wide(576),
        ],
        compiler_params=pltpu.CompilerParams(
            collective_id=0, has_side_effects=True, vmem_limit_bytes=67043328
        ),
        cost_estimate=pl.CostEstimate(flops=1 << 34, bytes_accessed=32 << 20, transcendentals=1 << 22),
        name="layer",
    )(*shards, dino, siglip, *gains)


def one_hot(per_device):
    width = 64 * per_device
    held = lax.broadcasted_iota(jnp.int32, (width, width), 1)
    slot = jnp.where(held < 512, held // 8, held - 512)
    row = jnp.where(held < 512, held % 8, 8)
    xh, c, z, y = slot % 2, (slot // 2) % 2, (slot // 4) % 8, slot // 32
    natural = (((y * XH + xh) * Z + z) * C + c) * per_device + row
    return (lax.broadcasted_iota(jnp.int32, (width, width), 0) == natural).astype(BF)


def normed(x, gain):
    center = x - jnp.mean(x, axis=-1, keepdims=True)
    spread = jnp.mean(center * center, axis=-1, keepdims=True)
    return (center * lax.rsqrt(spread + EPS) * gain).astype(BF)


def dot(a, b):
    return jnp.dot(a, b, preferred_element_type=F32)


def dot_t(a, b):
    return lax.dot_general(a, b, (((1,), (1,)), ((), ())), preferred_element_type=F32)


def gelu(x, approx):
    if approx:
        return jax.nn.gelu(x, approximate=True)
    half = 0.5 * x
    return half + half * lax.erf(x * math.sqrt(0.5))


def local(
    dino_tokens,
    siglip_tokens,
    dino_norm_one,
    dino_qkv,
    dino_out,
    dino_norm_two,
    dino_up,
    dino_down,
    siglip_norm_one,
    siglip_qkv,
    siglip_out,
    siglip_norm_two,
    siglip_up,
    siglip_down,
):
    shards = [
        dino_qkv.transpose(1, 0, 2), dino_out.T, dino_up, dino_down.T,
        siglip_qkv.reshape(9, -1), siglip_out.T, siglip_up, siglip_down.T,
    ]
    gains = [g.reshape(1, -1) for g in (dino_norm_one, dino_norm_two, siglip_norm_one, siglip_norm_two)]
    dino_result, siglip_result = layer(shards, dino_tokens, siglip_tokens.T, *gains)
    return (dino_result, siglip_result.T)


def solution(mesh):
    in_specs = (
        P("dp", "mp"),
        P("dp", "mp"),
        P(),
        P("dp", None, "mp"),
        P("mp", "dp"),
        P(),
        P("dp", "mp"),
        P("mp", "dp"),
        P(),
        P("dp", None, "mp"),
        P("mp", "dp"),
        P(),
        P("dp", "mp"),
        P("mp", "dp"),
    )
    out_specs = (P("dp", "mp"), P("dp", "mp"))
    return jax.shard_map(local, mesh=mesh, in_specs=in_specs, out_specs=out_specs, check_vma=False)
```
